128 devices in a mesh: row: 8 (over x, core), col: 16 (over z, y).
Axes of the slice: x: 4, y: 4, z: 4, core: 2. Of those that a mesh axis runs over, the one named last changes fastest.
Arguments:
- stored: float32 [16384, 16384], P('row', 'col'), as said below
Outputs:
- updated: float32 [16384, 16384], P('row', 'col')
- log_det: float32 [], replicated
Inputs may be any that keep to these rules, and one draw needn't show every extreme that they name: `stored`: read back into global order, the matrix is symmetric positive definite, with every eigenvalue at least 1.
All inputs are finite; a program needn't handle non-finite values.
Results may differ from the reference program's by a relative error of at most 0.0001.
Values sent between devices are 32-bit elements; how exact they have to be, the bound alone decides.
A program may use at most 256 MiB of HBM per device.

```python
import math
import jax
import jax.numpy as jnp
from jax import lax

N = 16384
NB = 512
PANELS = 2
N_ROW = 8
N_COL = 16


def to_storage(matrix):
    row_blocks = N // NB // N_ROW
    col_blocks = N // NB // N_COL
    shaped = matrix.reshape(row_blocks, N_ROW, NB, col_blocks, N_COL, NB)
    return shaped.transpose(1, 0, 2, 4, 3, 5).reshape(N, N)


def draw_stored(key, part):
    base_key = jax.random.fold_in(key, 7)
    first_key, second_key = jax.random.split(base_key)
    rank_count = N // 8
    factors = jax.random.normal(first_key, (N, rank_count), jnp.float32)
    weights = jnp.exp(jax.random.uniform(second_key, (rank_count,), jnp.float32, math.log(0.25), math.log(1.25)))
    scaled = factors * (weights / rank_count)[None, :]
    coupling = jnp.dot(scaled, factors.T, precision=lax.Precision.HIGHEST, preferred_element_type=jnp.float32)
    coupling = 0.5 * (coupling + coupling.T)
    return to_storage(coupling + jnp.eye(N, dtype=jnp.float32))


def setup_inputs(seed: int = 0) -> dict:
    key_of = jax.random.split(jax.random.key(seed), 2)
    stored = draw_stored(jax.random.fold_in(key_of[1], 71), 0)
    return dict(stored=stored)


def unpermute(stored):
    row_blocks = N // NB // N_ROW
    col_blocks = N // NB // N_COL
    shaped = stored.reshape(N_ROW, row_blocks, NB, N_COL, col_blocks, NB)
    return shaped.transpose(1, 0, 2, 4, 3, 5).reshape(N, N)

def permute(matrix):
    row_blocks = N // NB // N_ROW
    col_blocks = N // NB // N_COL
    shaped = matrix.reshape(row_blocks, N_ROW, NB, col_blocks, N_COL, NB)
    return shaped.transpose(1, 0, 2, 4, 3, 5).reshape(N, N)

def reference(stored):
    matrix = unpermute(stored)
    identity = jnp.eye(NB, dtype=jnp.float32)
    log_total = jnp.zeros((), jnp.float32)
    for number in range(PANELS):
        start = number * NB
        finish = start + NB
        factor = jnp.linalg.cholesky(matrix[start:finish, start:finish])
        inverse = jax.scipy.linalg.solve_triangular(factor, identity, lower=True)
        solved = jnp.dot(matrix[finish:, start:finish].astype(jnp.float32), inverse.T.astype(jnp.float32), precision=lax.Precision.HIGHEST, preferred_element_type=jnp.float32)
        log_total = log_total + 2.0 * jnp.sum(jnp.log(jnp.diagonal(factor)))
        update = jnp.dot(solved.astype(jnp.float32), solved.T.astype(jnp.float32), precision=lax.Precision.HIGHEST, preferred_element_type=jnp.float32)
        matrix = matrix.at[finish:, finish:].add(-update)
        matrix = matrix.at[start:finish, start:finish].set(factor)
        matrix = matrix.at[finish:, start:finish].set(solved)
        matrix = matrix.at[start:finish, finish:].set(0.0)
    return (permute(matrix), log_total)
```

```python
import jax
import jax.numpy as jnp
from jax import lax
from jax.experimental import pallas as pl
from jax.experimental.pallas import tpu as pltpu
from jax.sharding import PartitionSpec as P

NB = 512
TB = 128
CH = 32
F32 = jnp.float32
BF = jnp.bfloat16
HI = lax.Precision.HIGHEST
MESH = pl.DeviceIdType.MESH

TREES = (
    (1, 27, 41, 48, 48, 39, 49, 64, 64, 53, 65, 80, 48, 36, 49, 64),
    (2, 48, 64, 48, 23, 40, 58, 46, 35, 50, 66, 50, 48, 64, 80, 64),
    (4, 48, 38, 30, 48, 64, 52, 33, 64, 80, 68, 53, 48, 64, 52, 45),
    (8, 48, 64, 48, 48, 64, 80, 64, 44, 56, 72, 56, 29, 43, 58, 34),
)
MAXDEPTH = 5
SKEW = 2
NX = 16
ND = 4
NA = 16
LAG = 5 + 3 * SKEW


def lookup(table, position):
    value = jnp.int32(table[0])
    for index in range(1, len(table)):
        value = jnp.where(position == index, jnp.int32(table[index]), value)
    return value


def comm_kernel(stored, arow_out, acol_out, diag_out, arow, acol, diag,
                lsem, x_recv, xp_recv, x_send, xp_send, p_recv, p_send, d_recv, d_send):
    row = lax.axis_index("row")
    col = lax.axis_index("col")
    x, core = row // 2, row % 2
    z, y = col // 4, col % 4
    partner = (x * 2 + (1 - core), col)
    x_next = (((x + 1) % 4) * 2 + core, col)
    x_prev = (((x + 3) % 4) * 2 + core, col)
    plane = (
        (row, z * 4 + (y + 1) % 4),
        (row, ((z + 1) % 4) * 4 + y),
        (row, z * 4 + (y + 3) % 4),
        (row, ((z + 3) % 4) * 4 + y),
    )
    barrier = pltpu.get_barrier_semaphore()
    for other in (partner, x_next, x_prev) + plane:
        pl.semaphore_signal(barrier, inc=1, device_id=other, device_id_type=MESH)

    @pl.when(x == 0)
    def _():
        own = pltpu.make_async_copy(stored.at[pl.ds(0, NB), :], acol.at[core], lsem.at[0])
        own.start()
        own.wait()

    for k in range(2):
        @pl.when(col == k)
        def _():
            own = pltpu.make_async_copy(stored.at[:, pl.ds(0, NB)], arow.at[k], lsem.at[1])
            own.start()
            own.wait()

    pl.semaphore_wait(barrier, 7)

    def x_view(which, d, i):
        rows = pl.multiple_of((2 * (i % 8) + d) * CH, CH)
        return acol.at[which, pl.ds(rows, CH), pl.ds(pl.multiple_of((i // 8) * NB, NB), NB)]

    def x_copy(d, i):
        view = x_view(core, d, i)
        return pltpu.make_async_remote_copy(
            view, view, x_send.at[d], x_recv.at[d, i], device_id=(x_next, x_prev)[d], device_id_type=MESH)

    def xp_copy(d, i, which):
        view = x_view(which, d, i)
        return pltpu.make_async_remote_copy(
            view, view, xp_send.at[d], xp_recv.at[d, i], device_id=partner, device_id_type=MESH)

    def p_view(k, t, j):
        rows = pl.multiple_of((4 * (j - ND) + t) * CH, CH)
        return arow.at[k, pl.ds(rows, CH), :]

    def d_view(slot, t, j):
        return diag.at[slot, pl.ds(pl.multiple_of((4 * j + t) * CH, CH), CH), :]

    def d_source(which, t, j):
        return acol.at[which, pl.ds(pl.multiple_of((4 * j + t) * CH, CH), CH), pl.ds(0, NB)]

    def p_copy(src, dst, k, t, j, way):
        return pltpu.make_async_remote_copy(
            src, dst, p_send.at[k, t, way], p_recv.at[k, t, j], device_id=plane[way], device_id_type=MESH)

    def d_copy(slot, k, t, j):
        view = d_view(slot, t, j)
        return pltpu.make_async_remote_copy(
            view, view, d_send.at[k, t], d_recv.at[k, t, j], device_id=partner, device_id_type=MESH)

    codes = []
    for k in range(2):
        position = z * 4 + (y + 4 - k) % 4
        codes.append([lookup(TREES[t], position) for t in range(4)])
    steps = LAG + ND + NA + SKEW * MAXDEPTH

    def step(s, _):
        for d in range(2):
            distance = x if d == 0 else (4 - x) % 4
            i = s - SKEW * distance

            @pl.when((i >= 0) & (i < NX))
            def _():
                @pl.when(distance > 0)
                def _():
                    x_copy(d, i).wait_recv()

                @pl.when(i > 0)
                def _():
                    xp_copy(d, i - 1, core).wait_send()

                @pl.when((i > 0) & (distance < 3))
                def _():
                    x_copy(d, i - 1).wait_send()

                @pl.when(distance < 3)
                def _():
                    x_copy(d, i).start()

                xp_copy(d, i, core).start()

            h = i - SKEW

            @pl.when((h >= 0) & (h < NX))
            def _():
                xp_copy(d, h, 1 - core).wait_recv()

        for k in range(2):
            slot = core + k
            has_diag = (core == 0) if k == 0 else (core >= 0)
            for t in range(4):
                depth = codes[k][t] // 16
                mask = codes[k][t] % 16
                j = s - LAG - SKEW * depth
                in_diag = (j >= 0) & (j < ND) & has_diag
                in_rows = (j >= ND) & (j < ND + NA)
                active = in_diag | in_rows
                started = (j > 0) & active & ((j > ND) | has_diag)

                @pl.when(active & (depth > 0))
                def _():
                    p_copy(p_view(k, t, ND), p_view(k, t, ND), k, t, j, 0).wait_recv()

                for way in range(4):
                    child = (mask // (1 << way)) % 2 == 1

                    @pl.when(started & child)
                    def _():
                        p_copy(p_view(k, t, ND), p_view(k, t, ND), k, t, j - 1, way).wait_send()

                    @pl.when(in_rows & child)
                    def _():
                        p_copy(p_view(k, t, j), p_view(k, t, j), k, t, j, way).start()

                    @pl.when(in_diag & child & (depth == 0))
                    def _():
                        p_copy(d_source(core, t, j), d_view(slot, t, j), k, t, j, way).start()

                    @pl.when(in_diag & child & (depth > 0))
                    def _():
                        p_copy(d_view(slot, t, j), d_view(slot, t, j), k, t, j, way).start()

                @pl.when(in_diag & (depth > 0))
                def _():
                    @pl.when(j > 0)
                    def _():
                        d_copy(slot, k, t, j - 1).wait_send()
                    d_copy(slot, k, t, j).start()
        return 0

    lax.fori_loop(0, steps, step, 0)

    for d in range(2):
        distance = x if d == 0 else (4 - x) % 4
        xp_copy(d, NX - 1, core).wait_send()

        @pl.when(distance < 3)
        def _():
            x_copy(d, NX - 1).wait_send()
    for k in range(2):
        source = col == k
        away = col != k
        for t in range(4):
            mask = codes[k][t] % 16
            for way in range(4):
                @pl.when((mask // (1 << way)) % 2 == 1)
                def _():
                    p_copy(p_view(k, t, ND), p_view(k, t, ND), k, t, ND + NA - 1, way).wait_send()
            if k == 0:
                sends, gets = (core == 0) & away, (core == 1) & away
            else:
                sends, gets = away, away

            @pl.when(sends)
            def _():
                d_copy(0, k, t, 0).wait_send()

            @pl.when(gets)
            def _():
                for j in range(ND):
                    d_copy(0, k, t, j).wait_recv()

    @pl.when(col == 0)
    def _():
        diag[0] = acol[0, :, pl.ds(0, NB)]

    @pl.when(col == 1)
    def _():
        diag[1] = acol[0, :, pl.ds(0, NB)]
        diag[2] = acol[1, :, pl.ds(0, NB)]

    outs = [
        pltpu.make_async_copy(arow, arow_out, lsem.at[0]),
        pltpu.make_async_copy(acol, acol_out, lsem.at[1]),
    ]
    for copy in outs:
        copy.start()
    for copy in outs:
        copy.wait()
    last = pltpu.make_async_copy(diag, diag_out, lsem.at[2])
    last.start()
    last.wait()


def gather(stored):
    rows, cols = stored.shape
    shapes = ((2, rows, NB), (2, NB, cols), (3, NB, NB))
    dma = pltpu.SemaphoreType.DMA
    return pl.pallas_call(
        comm_kernel,
        name="gather_panels",
        out_shape=tuple(jax.ShapeDtypeStruct(s, F32) for s in shapes),
        in_specs=[pl.BlockSpec(memory_space=pl.ANY)],
        out_specs=(pl.BlockSpec(memory_space=pl.ANY),) * 3,
        scratch_shapes=[pltpu.VMEM(s, F32) for s in shapes]
        + [
            dma((3,)),
            dma((2, NX)),
            dma((2, NX)),
            dma((2,)),
            dma((2,)),
            dma((2, 4, ND + NA)),
            dma((2, 4, 4)),
            dma((2, 4, ND)),
            dma((2, 4)),
        ],
        compiler_params=pltpu.CompilerParams(
            collective_id=0, has_side_effects=True, vmem_limit_bytes=60 << 20),
    )(stored)


def spread(value, k):
    return jnp.broadcast_to(value[k : k + 1, :], (8, 128))


def split3(value):
    high = value.astype(BF)
    rest = value - high.astype(F32)
    middle = rest.astype(BF)
    low = (rest - middle.astype(F32)).astype(BF)
    return high, middle, low


def split2(value):
    high = value.astype(BF)
    return high, (value - high.astype(F32)).astype(BF)


def factor_tile(t, ld):
    sub = lax.broadcasted_iota(jnp.int32, (8, 128), 0)
    for p in range(8):
        r0 = 16 * p
        r = [[t[r0 + 8 * g : r0 + 8 * g + 8, 128 * h : 128 * h + 128] for h in range(2)] for g in range(2)]
        top = [jnp.broadcast_to(r[0][0][:, r0 + j : r0 + j + 1], (8, 128)) for j in range(8)]
        bot = [jnp.broadcast_to(r[1][0][:, r0 + j : r0 + j + 1], (8, 128)) for j in range(16)]
        piv = [jnp.ones((8, 128), F32), jnp.ones((8, 128), F32)]
        for k in range(16):
            g, kk = divmod(k, 8)
            pv = spread(top[k] if g == 0 else bot[k], kk)
            inv = 1.0 / pv
            piv[g] = jnp.where(sub == kk, pv, piv[g])
            mb = bot[k] * inv
            mt = top[k] * inv if g == 0 else None
            for j in range(k + 1, 16):
                s = spread(top[k], j) if j < 8 else spread(bot[k], j - 8)
                bot[j] = bot[j] - mb * s
                if j < 8:
                    top[j] = top[j] - mt * s
            for h in range(2):
                u = spread(r[g][h], kk)
                if g == 0:
                    r[0][h] = r[0][h] - jnp.where(sub > kk, mt, 0.0) * u
                    r[1][h] = r[1][h] - mb * u
                else:
                    r[1][h] = r[1][h] - jnp.where(sub > kk, mb, 0.0) * u
        ld[...] += jnp.log(piv[0]) + jnp.log(piv[1])
        rows = []
        for g in range(2):
            rs = lax.rsqrt(piv[g])
            rows.append([r[g][h] * rs for h in range(2)])
            for h in range(2):
                t[r0 + 8 * g : r0 + 8 * g + 8, 128 * h : 128 * h + 128] = rows[g][h]
        if p < 7:
            uh, um, ul = split3(jnp.concatenate([rows[0][0], rows[1][0]], 0))
            wh, wm, wl = split3(jnp.concatenate([rows[0][1], rows[1][1]], 0))
            lhs = jnp.concatenate([uh, uh, um, uh, ul, um], 0)
            rhs = jnp.concatenate(
                [jnp.concatenate([uh, um, uh, ul, uh, um], 0), jnp.concatenate([wh, wm, wh, wl, wh, wm], 0)], 1)
            upd = lax.dot_general(lhs, rhs, (((0,), (0,)), ((), ())), preferred_element_type=F32)
            t[r0 + 16 :, :] -= upd[r0 + 16 :, :]


def factor_block(b, t, ud, ld):
    ri = lax.broadcasted_iota(jnp.int32, (TB, TB), 0)
    ci = lax.broadcasted_iota(jnp.int32, (TB, TB), 1)
    n = NB // TB

    def step(blk, _):
        base = pl.multiple_of(blk * TB, TB)
        rows = pl.ds(base, TB)
        t[:, :TB] = b[rows, rows]
        t[:, TB:] = jnp.where(ri == ci, 1.0, 0.0)
        factor_tile(t, ld)
        w = jnp.where(ri >= ci, t[:, TB:], 0.0)
        ud[blk] = jnp.where(ri <= ci, t[:, :TB], 0.0)
        b[rows, :] = jnp.dot(w, b[rows, :], precision=HI, preferred_element_type=F32)
        b[rows, rows] = w

        def trail(i, _):
            ir = pl.ds(pl.multiple_of(i * TB, TB), TB)
            b[ir, rows] = jnp.zeros((TB, TB), F32)
            ut = b[rows, ir].T
            b[ir, :] -= jnp.dot(ut, b[rows, :], precision=HI, preferred_element_type=F32)
            return 0

        lax.fori_loop(blk + 1, n, trail, 0)
        return 0

    lax.fori_loop(0, n, step, 0)


def lower_tiles(b):
    ri = lax.broadcasted_iota(jnp.int32, (NB, NB), 0) // TB
    ci = lax.broadcasted_iota(jnp.int32, (NB, NB), 1) // TB
    return jnp.where(ri >= ci, b, 0.0)


def factor_kernel(diag, v0, v1, u01, b0, b1, ud0, ud1, log_det, s11, t, ld):
    ld[...] = jnp.zeros_like(ld)
    b0[...] = diag[0]
    factor_block(b0, t, ud0, ld)
    v0[...] = lower_tiles(b0[...])
    u01[...] = jnp.dot(v0[...], diag[1], precision=HI, preferred_element_type=F32)
    s11[...] = u01[...].T
    b1[...] = diag[2] - jnp.dot(s11[...], u01[...], precision=HI, preferred_element_type=F32)
    factor_block(b1, t, ud1, ld)
    v1[...] = lower_tiles(b1[...])
    log_det[...] = jnp.broadcast_to(jnp.sum(ld[...], axis=0, keepdims=True), (8, 128))


def factor(diag):
    square = jax.ShapeDtypeStruct((NB, NB), F32)
    tiles = jax.ShapeDtypeStruct((NB // TB, TB, TB), F32)
    vmem = pl.BlockSpec(memory_space=pltpu.VMEM)
    return pl.pallas_call(
        factor_kernel,
        name="factor_leading",
        out_shape=(square,) * 5 + (tiles,) * 2 + (jax.ShapeDtypeStruct((8, 128), F32),),
        in_specs=[vmem],
        out_specs=(vmem,) * 8,
        scratch_shapes=[pltpu.VMEM((NB, NB), F32), pltpu.VMEM((TB, 2 * TB), F32), pltpu.VMEM((8, 128), F32)],
        compiler_params=pltpu.CompilerParams(vmem_limit_bytes=60 << 20),
    )(diag)


def mul3(a, b, contract=((1,), (0,))):
    dims = (contract, ((), ()))
    dot = lambda p, q: lax.dot_general(p, q, dims, preferred_element_type=F32)
    return dot(a[0], b[0]) + (dot(a[0], b[1]) + dot(a[1], b[0]))


BT = ((1,), (1,))


def lower_factor(b, ud, out, i0, j0):
    n = NB // TB
    for i in range(n):
        for j in range(n):
            if i > j:
                tile = b[TB * j : TB * j + TB, TB * i : TB * i + TB].T
            elif i == j:
                tile = ud[i].T
            else:
                tile = jnp.zeros((TB, TB), F32)
            out[i0 + TB * i : i0 + TB * i + TB, j0 + TB * j : j0 + TB * j + TB] = tile


def update_kernel(m, arow, acol, v0, v1, u01, b0, b1, ud0, ud1, out, yh, yl, vh, vl, p):
    step = pl.program_id(0)
    row = lax.axis_index("row")
    col = lax.axis_index("col")

    @pl.when(step == 0)
    def _():
        for slot, ref in enumerate((v0, v1, u01)):
            vh[slot], vl[slot] = split2(ref[...])
        for c in range(2):
            cols = pl.ds(c * NB, NB)
            y0 = mul3((vh[0], vl[0]), split2(acol[0, :, cols]))
            y0s = split2(y0)
            yh[:NB, cols], yl[:NB, cols] = y0s
            rest = acol[1, :, cols] - mul3((vh[2], vl[2]), y0s, ((0,), (0,)))
            yh[NB:, cols], yl[NB:, cols] = split2(mul3((vh[1], vl[1]), split2(rest)))

    p0 = mul3(split2(arow[0]), (vh[0], vl[0]), BT)
    p0s = split2(p0)
    rest = arow[1] - mul3(p0s, (vh[2], vl[2]))
    p1 = mul3(split2(rest), (vh[1], vl[1]), BT)
    p1s = split2(p1)
    p[0], p[1] = p0, p1
    for c in range(2):
        cols = pl.ds(c * NB, NB)
        out[:, cols] = m[:, cols] - (
            mul3(p0s, (yh[:NB, cols], yl[:NB, cols])) + mul3(p1s, (yh[NB:, cols], yl[NB:, cols])))

    first = step == 0

    @pl.when(first & (row < 2))
    def _():
        out[...] = jnp.zeros_like(out)

    @pl.when((col == 0) & ~(first & (row == 0)))
    def _():
        out[:, pl.ds(0, NB)] = p[0]

    @pl.when((col == 1) & ~(first & (row < 2)))
    def _():
        out[:, pl.ds(0, NB)] = p[1]

    @pl.when((col == 0) & first & (row == 0))
    def _():
        lower_factor(b0, ud0, out, 0, 0)

    @pl.when((col == 1) & first & (row == 1))
    def _():
        lower_factor(b1, ud1, out, 0, 0)


def update(stored, arow, acol, v0, v1, u01, b0, b1, ud0, ud1):
    rows, cols = stored.shape
    whole = lambda a: pl.BlockSpec(a.shape, lambda i: (0,) * a.ndim, pipeline_mode=pl.Buffered(1))
    return pl.pallas_call(
        update_kernel,
        name="update_remaining",
        grid=(rows // NB,),
        out_shape=jax.ShapeDtypeStruct(stored.shape, F32),
        in_specs=[
            pl.BlockSpec((NB, cols), lambda i: (i, 0)),
            pl.BlockSpec((2, NB, NB), lambda i: (0, i, 0)),
        ]
        + [whole(a) for a in (acol, v0, v1, u01, b0, b1, ud0, ud1)],
        out_specs=pl.BlockSpec((NB, cols), lambda i: (i, 0)),
        scratch_shapes=[
            pltpu.VMEM((2 * NB, cols), BF),
            pltpu.VMEM((2 * NB, cols), BF),
            pltpu.VMEM((3, NB, NB), BF),
            pltpu.VMEM((3, NB, NB), BF),
            pltpu.VMEM((2, NB, NB), F32),
        ],
        compiler_params=pltpu.CompilerParams(vmem_limit_bytes=60 << 20),
    )(stored, arow, acol, v0, v1, u01, b0, b1, ud0, ud1)


def per_device(stored):
    arow, acol, diag = gather(stored)
    v0, v1, u01, b0, b1, ud0, ud1, log_det = factor(diag)
    updated = update(stored, arow, acol, v0, v1, u01, b0, b1, ud0, ud1)
    return updated, log_det[0, 0]


def solution(mesh):
    placed = (P("row", "col"),)
    return jax.shard_map(
        per_device, mesh=mesh, in_specs=placed, out_specs=(P("row", "col"), P()), check_vma=False
    )
```

```python
import jax
import jax.numpy as jnp
from jax import lax
from jax.experimental import pallas as pl
from jax.experimental.pallas import tpu as pltpu
from jax.sharding import PartitionSpec as P

NB = 512
TB = 128
CH = 32
F32 = jnp.float32
BF = jnp.bfloat16
HI = lax.Precision.HIGHEST
MESH = pl.DeviceIdType.MESH

TREES = (
    (1, 27, 41, 48, 48, 39, 49, 64, 64, 53, 65, 80, 48, 36, 49, 64),
    (2, 48, 64, 48, 23, 40, 58, 46, 35, 50, 66, 50, 48, 64, 80, 64),
    (4, 48, 38, 30, 48, 64, 52, 33, 64, 80, 68, 53, 48, 64, 52, 45),
    (8, 48, 64, 48, 48, 64, 80, 64, 44, 56, 72, 56, 29, 43, 58, 34),
)
MAXDEPTH = 5
SKEW = 3
NX = 16
NQ = 20
D0, D1 = 4, 8
EARLY = 3
DSTEP = 11
LATE = 18
XDELAY = 15
FIRST = 33
SLOW = 6


def lookup(table, position):
    value = jnp.int32(table[0])
    for index in range(1, len(table)):
        value = jnp.where(position == index, jnp.int32(table[index]), value)
    return value


def remote(src, dst, send, recv, device):
    return pltpu.make_async_remote_copy(src, dst, send, recv, device_id=device, device_id_type=MESH)


def panel_kernel(stored, arow_out, acol_out, b_out, u01_out, ud_out, ld_out,
                 buf, other, dx, b, u01, ud, ld, t, s11,
                 lsem, x_recv, xp_recv, x_send, xp_send, p_recv, p_send, d_recv, d_send):
    row = lax.axis_index("row")
    col = lax.axis_index("col")
    x, core = row // 2, row % 2
    z, y = col // 4, col % 4
    partner = (x * 2 + (1 - core), col)
    x_next = (((x + 1) % 4) * 2 + core, col)
    x_prev = (((x + 3) % 4) * 2 + core, col)
    plane = (
        (row, z * 4 + (y + 1) % 4),
        (row, ((z + 1) % 4) * 4 + y),
        (row, z * 4 + (y + 3) % 4),
        (row, ((z + 3) % 4) * 4 + y),
    )
    slab = jnp.where(col < 2, col, 2)
    barrier = pltpu.get_barrier_semaphore()
    for device in (partner, x_next, x_prev) + plane:
        pl.semaphore_signal(barrier, inc=1, device_id=device, device_id_type=MESH)

    @pl.when(x == 0)
    def _():
        own = [
            pltpu.make_async_copy(
                stored.at[pl.ds(0, NB), pl.ds(0, NB)], buf.at[slab, pl.ds(NB, NB), :], lsem.at[0]),
            pltpu.make_async_copy(
                stored.at[pl.ds(0, NB), pl.ds(NB, NB)], buf.at[2, pl.ds(2 * NB, NB), :], lsem.at[1]),
        ]
        for copy in own:
            copy.start()
        own[0].wait()

    for k in range(2):
        @pl.when(col == k)
        def _():
            own = [
                pltpu.make_async_copy(
                    stored.at[pl.ds(0, NB), pl.ds(0, NB)], buf.at[k, pl.ds(0, NB), :], lsem.at[2]),
                pltpu.make_async_copy(
                    stored.at[pl.ds(NB, 3 * NB), pl.ds(0, NB)], buf.at[k, pl.ds(2 * NB, 3 * NB), :], lsem.at[3]),
            ]
            for copy in own:
                copy.start()
            own[0].wait()

    pl.semaphore_wait(barrier, 7)

    def loaded():
        @pl.when(x == 0)
        def _():
            pltpu.make_async_copy(
                stored.at[pl.ds(0, NB), pl.ds(NB, NB)], buf.at[2, pl.ds(2 * NB, NB), :], lsem.at[1]).wait()

        for k in range(2):
            @pl.when(col == k)
            def _():
                pltpu.make_async_copy(
                    stored.at[pl.ds(NB, 3 * NB), pl.ds(0, NB)], buf.at[k, pl.ds(2 * NB, 3 * NB), :], lsem.at[3]).wait()

    def x_rows(d, i):
        return (2 * (i % 8) + d) * CH

    def x_view(d, i):
        second = i // 8
        start = pl.multiple_of(NB + NB * second + x_rows(d, i), CH)
        return buf.at[slab + second * (2 - slab), pl.ds(start, CH), :]

    def x_copy(d, i):
        view = x_view(d, i)
        return remote(view, view, x_send.at[d], x_recv.at[d, i], (x_next, x_prev)[d])

    def xp_copy(d, i):
        target = other.at[i // 8, pl.ds(pl.multiple_of(x_rows(d, i), CH), CH), :]
        return remote(x_view(d, i), target, xp_send.at[d], xp_recv.at[d, i], partner)

    def p_copy(k, t, q, way):
        view = buf.at[k, pl.ds(pl.multiple_of((4 * q + t) * CH, CH), CH), :]
        return remote(view, view, p_send.at[k, t, way], p_recv.at[k, t, q], plane[way])

    def d_copy(k, t, q):
        view = buf.at[k, pl.ds(pl.multiple_of((4 * q + t) * CH, CH), CH), :]
        target = dx.at[k * (1 - core), pl.ds(pl.multiple_of((4 * (q - D0) + t) * CH, CH), CH), :]
        return remote(view, target, d_send.at[k, t], d_recv.at[k, t, q - D0], partner)

    depths, children = [], []
    for k in range(2):
        position = z * 4 + (y + 4 - k) % 4
        codes = [lookup(TREES[t], position) for t in range(4)]
        depths.append([code // 16 for code in codes])
        children.append([[(code // (1 << way)) % 2 == 1 for way in range(4)] for code in codes])
    has_diag = [core == 0, core >= 0]

    def step(s, _):
        for d in range(2):
            distance = x if d == 0 else (4 - x) % 4
            v = s - SKEW * distance - XDELAY * core
            w = s - SLOW * distance - XDELAY * core
            i = jnp.where(v < 8, v, 8 + (w - LATE) // EARLY)
            on_time = (v < 8) | ((w >= LATE) & (w % EARLY == 0))

            @pl.when((v >= 0) & (i < NX) & on_time)
            def _():
                @pl.when(distance > 0)
                def _():
                    x_copy(d, i).wait_recv()

                @pl.when(i > 0)
                def _():
                    xp_copy(d, i - 1).wait_send()

                xp_copy(d, i).start()

                @pl.when(distance < 3)
                def _():
                    @pl.when(i > 0)
                    def _():
                        x_copy(d, i - 1).wait_send()

                    x_copy(d, i).start()

        for k in range(2):
            for t in range(4):
                v = s - SKEW * depths[k][t]
                late = s - SLOW * depths[k][t]
                w = (late - LATE) // EARLY
                q_late = 8 + w
                if k == 1:
                    q_late = q_late - core * jnp.where(w < 3, 0, jnp.where(w < 7, 7, 4))
                q = jnp.where(v < DSTEP, v // EARLY, jnp.where(v < LATE, D0 + (v - DSTEP) // 2, q_late))
                early = (v >= 0) & (v < EARLY * D0) & (v % EARLY == 0)
                diag = (v >= DSTEP) & (v < LATE) & ((v - DSTEP) % 2 == 0) & (core == 0)
                active = early | diag | ((late >= LATE) & (late % EARLY == 0) & (q < NQ))
                in_diag = (q >= D0) & (q < D1)

                @pl.when(active)
                def _():
                    @pl.when(depths[k][t] > 0)
                    def _():
                        p_copy(k, t, q, 0).wait_recv()

                    for way in range(4):
                        @pl.when(children[k][t][way])
                        def _():
                            @pl.when(q > 0)
                            def _():
                                p_copy(k, t, q - 1, way).wait_send()

                            p_copy(k, t, q, way).start()

                    @pl.when(in_diag)
                    def _():
                        @pl.when(q > D0)
                        def _():
                            d_copy(k, t, q - 1).wait_send()

                        d_copy(k, t, q).start()
        return 0

    def take(k):
        for t in range(4):
            for j in range(D1 - D0):
                d_copy(k, t, D0 + j).wait_recv()

    lax.fori_loop(0, 12, step, 0)
    loaded()
    lax.fori_loop(12, FIRST, step, 0)

    ri = lax.broadcasted_iota(jnp.int32, (TB, TB), 0)
    ci = lax.broadcasted_iota(jnp.int32, (TB, TB), 1)
    n = NB // TB
    ld[...] = jnp.zeros_like(ld)

    @pl.when(core == 0)
    def _():
        b[0] = buf[0, pl.ds(NB, NB), :]

    @pl.when(core == 1)
    def _():
        take(0)
        b[0] = dx[0]

    def tile(g, _):
        half, blk = g // n, g % n

        @pl.when(g == n)
        def _():
            v0 = lower_tiles(b[0])

            @pl.when(core == 0)
            def _():
                take(1)
                u01[...] = jnp.dot(v0, buf[1, pl.ds(NB, NB), :], precision=HI, preferred_element_type=F32)
                b[1] = dx[0]

            @pl.when(core == 1)
            def _():
                take(1)
                u01[...] = jnp.dot(v0, dx[1], precision=HI, preferred_element_type=F32)
                b[1] = buf[1, pl.ds(NB, NB), :]

            s11[...] = u01[...].T
            b[1] -= jnp.dot(s11[...], u01[...], precision=HI, preferred_element_type=F32)

        base = pl.multiple_of(blk * TB, TB)
        rows = pl.ds(base, TB)
        t[:, :TB] = b[half, rows, rows]
        t[:, TB:] = jnp.where(ri == ci, 1.0, 0.0)
        begin = jnp.where(g < n, 3 * g, n + 2 * g)
        finish = begin + jnp.where((g < n) | (g == 2 * n - 1), 3, 2)

        def late_step(u, _):
            return step(FIRST + EARLY * u, 0)

        factor_tile(t, ld, lambda: late_step(begin, 0))
        w = jnp.where(ri >= ci, t[:, TB:], 0.0)
        ud[g] = jnp.where(ri <= ci, t[:, :TB], 0.0)
        b[half, rows, :] = mul6(split3(w), split3(b[half, rows, :]))
        b[half, rows, rows] = w
        done = b[half, rows, :]
        change = mul6(split3(done.T), split3(done))
        for i in range(1, n):
            @pl.when(blk < i)
            def _():
                b[half, TB * i : TB * i + TB, rows] = jnp.zeros((TB, TB), F32)
                b[half, TB * i : TB * i + TB, :] -= change[TB * i : TB * i + TB, :]

        lax.fori_loop(begin + 1, finish, late_step, 0)
        return 0

    lax.fori_loop(0, 2 * n, tile, 0)

    for d in range(2):
        distance = x if d == 0 else (4 - x) % 4
        xp_copy(d, NX - 1).wait_send()
        for i in range(NX):
            xp_copy(d, i).wait_recv()

        @pl.when(distance < 3)
        def _():
            x_copy(d, NX - 1).wait_send()
    for k in range(2):
        for t in range(4):
            for way in range(4):
                @pl.when(children[k][t][way])
                def _():
                    p_copy(k, t, NQ - 1, way).wait_send()

            @pl.when(has_diag[k])
            def _():
                d_copy(k, t, D1 - 1).wait_send()

    first, second = pl.ds(0, NB), pl.ds(NB, NB)
    outs = [
        (buf.at[pl.ds(0, 2), first, :], arow_out.at[:, first, :]),
        (buf.at[pl.ds(0, 2), pl.ds(2 * NB, 3 * NB), :], arow_out.at[:, pl.ds(NB, 3 * NB), :]),
        (buf.at[slab, second, :], acol_out.at[core, :, first]),
        (buf.at[2, pl.ds(2 * NB, NB), :], acol_out.at[core, :, second]),
        (other.at[0], acol_out.at[1 - core, :, first]),
        (other.at[1], acol_out.at[1 - core, :, second]),
        (u01, u01_out),
        (ud, ud_out),
        (b, b_out),
        (ld, ld_out),
    ]
    copies = [pltpu.make_async_copy(src, dst, lsem.at[index]) for index, (src, dst) in enumerate(outs)]
    for copy in copies:
        copy.start()
    for copy in copies:
        copy.wait()


def panels(stored):
    rows, cols = stored.shape
    n = NB // TB
    outs = ((2, rows, NB), (2, NB, cols), (2, NB, NB), (NB, NB), (2 * n, TB, TB), (8, 128))
    scratch = ((3, rows + NB, NB), (2, NB, NB), (2, NB, NB), (2, NB, NB), (NB, NB), (2 * n, TB, TB), (8, 128),
               (TB, 2 * TB), (NB, NB))
    dma = pltpu.SemaphoreType.DMA
    return pl.pallas_call(
        panel_kernel,
        name="gather_and_factor",
        out_shape=tuple(jax.ShapeDtypeStruct(s, F32) for s in outs),
        in_specs=[pl.BlockSpec(memory_space=pl.ANY)],
        out_specs=(pl.BlockSpec(memory_space=pl.ANY),) * len(outs),
        scratch_shapes=[pltpu.VMEM(s, F32) for s in scratch]
        + [
            dma((10,)),
            dma((2, NX)),
            dma((2, NX)),
            dma((2,)),
            dma((2,)),
            dma((2, 4, NQ)),
            dma((2, 4, 4)),
            dma((2, 4, D1 - D0)),
            dma((2, 4)),
        ],
        compiler_params=pltpu.CompilerParams(
            collective_id=0, has_side_effects=True, vmem_limit_bytes=60 << 20),
    )(stored)


def spread(value, k):
    return jnp.broadcast_to(value[k : k + 1, :], (8, 128))


def split3(value):
    high = value.astype(BF)
    rest = value - high.astype(F32)
    middle = rest.astype(BF)
    low = (rest - middle.astype(F32)).astype(BF)
    return high, middle, low


def split2(value):
    high = value.astype(BF)
    return high, (value - high.astype(F32)).astype(BF)


def mul6(a, b):
    lhs = jnp.concatenate([a[0], a[0], a[1], a[0], a[2], a[1]], 1)
    rhs = jnp.concatenate([b[0], b[1], b[0], b[2], b[0], b[1]], 0)
    return jnp.dot(lhs, rhs, preferred_element_type=F32)


def factor_tile(t, ld, between):
    sub = lax.broadcasted_iota(jnp.int32, (8, 128), 0)
    for p in range(8):
        r0 = 16 * p
        r = [[t[r0 + 8 * g : r0 + 8 * g + 8, 128 * h : 128 * h + 128] for h in range(2)] for g in range(2)]
        top = [jnp.broadcast_to(r[0][0][:, r0 + j : r0 + j + 1], (8, 128)) for j in range(8)]
        bot = [jnp.broadcast_to(r[1][0][:, r0 + j : r0 + j + 1], (8, 128)) for j in range(16)]
        piv = [jnp.ones((8, 128), F32), jnp.ones((8, 128), F32)]
        for k in range(16):
            g, kk = divmod(k, 8)
            pv = spread(top[k] if g == 0 else bot[k], kk)
            inv = 1.0 / pv
            piv[g] = jnp.where(sub == kk, pv, piv[g])
            mb = bot[k] * inv
            mt = top[k] * inv if g == 0 else None
            for j in range(k + 1, 16):
                s = spread(top[k], j) if j < 8 else spread(bot[k], j - 8)
                bot[j] = bot[j] - mb * s
                if j < 8:
                    top[j] = top[j] - mt * s
            for h in range(2):
                u = spread(r[g][h], kk)
                if g == 0:
                    r[0][h] = r[0][h] - jnp.where(sub > kk, mt, 0.0) * u
                    r[1][h] = r[1][h] - mb * u
                else:
                    r[1][h] = r[1][h] - jnp.where(sub > kk, mb, 0.0) * u
        ld[...] += jnp.log(piv[0]) + jnp.log(piv[1])
        rows = []
        for g in range(2):
            rs = lax.rsqrt(piv[g])
            rows.append([r[g][h] * rs for h in range(2)])
            for h in range(2):
                t[r0 + 8 * g : r0 + 8 * g + 8, 128 * h : 128 * h + 128] = rows[g][h]
        if p < 7:
            uh, um, ul = split3(jnp.concatenate([rows[0][0], rows[1][0]], 0))
            wh, wm, wl = split3(jnp.concatenate([rows[0][1], rows[1][1]], 0))
            lhs = jnp.concatenate([uh, uh, um, uh, ul, um], 0)
            rhs = jnp.concatenate(
                [jnp.concatenate([uh, um, uh, ul, uh, um], 0), jnp.concatenate([wh, wm, wh, wl, wh, wm], 0)], 1)
            upd = lax.dot_general(lhs, rhs, (((0,), (0,)), ((), ())), preferred_element_type=F32)
            t[r0 + 16 :, :] -= upd[r0 + 16 :, :]
        if p == 3:
            between()


def lower_tiles(b):
    ri = lax.broadcasted_iota(jnp.int32, (NB, NB), 0) // TB
    ci = lax.broadcasted_iota(jnp.int32, (NB, NB), 1) // TB
    return jnp.where(ri >= ci, b, 0.0)


def mul3(a, b, contract=((1,), (0,))):
    dims = (contract, ((), ()))
    dot = lambda p, q: lax.dot_general(p, q, dims, preferred_element_type=F32)
    return dot(a[0], b[0]) + (dot(a[0], b[1]) + dot(a[1], b[0]))


BT = ((1,), (1,))


def lower_factor(k, b, ud, out):
    n = NB // TB
    for i in range(n):
        for j in range(n):
            if i > j:
                tile = b[k, TB * j : TB * j + TB, TB * i : TB * i + TB].T
            elif i == j:
                tile = ud[k * n + i].T
            else:
                tile = jnp.zeros((TB, TB), F32)
            out[TB * i : TB * i + TB, TB * j : TB * j + TB] = tile


def update_kernel(m, arow, acol, b, u01, ud, ld, out, log_det, yh, yl, vh, vl, p):
    step = pl.program_id(0)
    row = lax.axis_index("row")
    col = lax.axis_index("col")

    @pl.when(step == 0)
    def _():
        log_det[0, 0] = jnp.sum(ld[:, 0:1])
        for slot in range(2):
            vh[slot], vl[slot] = split2(lower_tiles(b[slot]))
        vh[2], vl[2] = split2(u01[...])
        for c in range(2):
            cols = pl.ds(c * NB, NB)
            y0 = mul3((vh[0], vl[0]), split2(acol[0, :, cols]))
            y0s = split2(y0)
            yh[:NB, cols], yl[:NB, cols] = y0s
            rest = acol[1, :, cols] - mul3((vh[2], vl[2]), y0s, ((0,), (0,)))
            yh[NB:, cols], yl[NB:, cols] = split2(mul3((vh[1], vl[1]), split2(rest)))

    p0 = mul3(split2(arow[0]), (vh[0], vl[0]), BT)
    p0s = split2(p0)
    rest = arow[1] - mul3(p0s, (vh[2], vl[2]))
    p1 = mul3(split2(rest), (vh[1], vl[1]), BT)
    p1s = split2(p1)
    p[0], p[1] = p0, p1
    for c in range(2):
        cols = pl.ds(c * NB, NB)
        out[:, cols] = m[:, cols] - (
            mul3(p0s, (yh[:NB, cols], yl[:NB, cols])) + mul3(p1s, (yh[NB:, cols], yl[NB:, cols])))

    first = step == 0

    @pl.when(first & (row < 2))
    def _():
        out[...] = jnp.zeros_like(out)

    @pl.when((col == 0) & ~(first & (row == 0)))
    def _():
        out[:, pl.ds(0, NB)] = p[0]

    @pl.when((col == 1) & ~(first & (row < 2)))
    def _():
        out[:, pl.ds(0, NB)] = p[1]

    @pl.when((col == 0) & first & (row == 0))
    def _():
        lower_factor(0, b, ud, out)

    @pl.when((col == 1) & first & (row == 1))
    def _():
        lower_factor(1, b, ud, out)


def update(stored, arow, acol, b, u01, ud, ld):
    rows, cols = stored.shape
    whole = lambda a: pl.BlockSpec(a.shape, lambda i: (0,) * a.ndim, pipeline_mode=pl.Buffered(1))
    return pl.pallas_call(
        update_kernel,
        name="update_remaining",
        grid=(rows // NB,),
        out_shape=(jax.ShapeDtypeStruct(stored.shape, F32), jax.ShapeDtypeStruct((1, 1), F32)),
        in_specs=[
            pl.BlockSpec((NB, cols), lambda i: (i, 0)),
            pl.BlockSpec((2, NB, NB), lambda i: (0, i, 0)),
        ]
        + [whole(a) for a in (acol, b, u01, ud, ld)],
        out_specs=(pl.BlockSpec((NB, cols), lambda i: (i, 0)), pl.BlockSpec(memory_space=pltpu.SMEM)),
        scratch_shapes=[
            pltpu.VMEM((2 * NB, cols), BF),
            pltpu.VMEM((2 * NB, cols), BF),
            pltpu.VMEM((3, NB, NB), BF),
            pltpu.VMEM((3, NB, NB), BF),
            pltpu.VMEM((2, NB, NB), F32),
        ],
        compiler_params=pltpu.CompilerParams(vmem_limit_bytes=60 << 20),
    )(stored, arow, acol, b, u01, ud, ld)


def per_device(stored):
    updated, log_det = update(stored, *panels(stored))
    return updated, log_det.reshape(())


def solution(mesh):
    placed = (P("row", "col"),)
    return jax.shard_map(
        per_device, mesh=mesh, in_specs=placed, out_specs=(P("row", "col"), P()), check_vma=False
    )
```

```python
import jax
import jax.numpy as jnp
from jax import lax
from jax.experimental import pallas as pl
from jax.experimental.pallas import tpu as pltpu
from jax.sharding import PartitionSpec as P

NB = 512
TB = 128
CH = 32
F32 = jnp.float32
BF = jnp.bfloat16
HI = lax.Precision.HIGHEST
MESH = pl.DeviceIdType.MESH

TREES = (
    (1, 27, 41, 48, 48, 39, 49, 64, 64, 53, 65, 80, 48, 36, 49, 64),
    (2, 48, 64, 48, 23, 40, 58, 46, 35, 50, 66, 50, 48, 64, 80, 64),
    (4, 48, 38, 30, 48, 64, 52, 33, 64, 80, 68, 53, 48, 64, 52, 45),
    (8, 48, 64, 48, 48, 64, 80, 64, 44, 56, 72, 56, 29, 43, 58, 34),
)
MAXDEPTH = 5
SKEW = 3
NX = 16
NQ = 20
D0, D1 = 4, 8
EARLY = 3
DSTEP = 11
LATE = 18
XDELAY = 15
FIRST = 33
SLOW = 6


def lookup(table, position):
    value = jnp.int32(table[0])
    for index in range(1, len(table)):
        value = jnp.where(position == index, jnp.int32(table[index]), value)
    return value


def remote(src, dst, send, recv, device):
    return pltpu.make_async_remote_copy(src, dst, send, recv, device_id=device, device_id_type=MESH)


def panel_kernel(stored, arow_out, acol_out, b_out, u01_out, ud_out, ld_out,
                 buf, other, dx, b, u01, ud, ld, t, s11,
                 lsem, x_recv, xp_recv, x_send, xp_send, p_recv, p_send, d_recv, d_send):
    row = lax.axis_index("row")
    col = lax.axis_index("col")
    x, core = row // 2, row % 2
    z, y = col // 4, col % 4
    partner = (x * 2 + (1 - core), col)
    x_next = (((x + 1) % 4) * 2 + core, col)
    x_prev = (((x + 3) % 4) * 2 + core, col)
    plane = (
        (row, z * 4 + (y + 1) % 4),
        (row, ((z + 1) % 4) * 4 + y),
        (row, z * 4 + (y + 3) % 4),
        (row, ((z + 3) % 4) * 4 + y),
    )
    slab = jnp.where(col < 2, col, 2)
    barrier = pltpu.get_barrier_semaphore()
    for device in (partner, x_next, x_prev) + plane:
        pl.semaphore_signal(barrier, inc=1, device_id=device, device_id_type=MESH)

    @pl.when(x == 0)
    def _():
        own = [
            pltpu.make_async_copy(
                stored.at[pl.ds(0, NB), pl.ds(0, NB)], buf.at[slab, pl.ds(NB, NB), :], lsem.at[0]),
            pltpu.make_async_copy(
                stored.at[pl.ds(0, NB), pl.ds(NB, NB)], buf.at[2, pl.ds(2 * NB, NB), :], lsem.at[1]),
        ]
        for copy in own:
            copy.start()
        own[0].wait()

    for k in range(2):
        @pl.when(col == k)
        def _():
            own = [
                pltpu.make_async_copy(
                    stored.at[pl.ds(0, NB), pl.ds(0, NB)], buf.at[k, pl.ds(0, NB), :], lsem.at[2]),
                pltpu.make_async_copy(
                    stored.at[pl.ds(NB, 3 * NB), pl.ds(0, NB)], buf.at[k, pl.ds(2 * NB, 3 * NB), :], lsem.at[3]),
            ]
            for copy in own:
                copy.start()
            own[0].wait()

    pl.semaphore_wait(barrier, 7)

    def loaded():
        @pl.when(x == 0)
        def _():
            pltpu.make_async_copy(
                stored.at[pl.ds(0, NB), pl.ds(NB, NB)], buf.at[2, pl.ds(2 * NB, NB), :], lsem.at[1]).wait()

        for k in range(2):
            @pl.when(col == k)
            def _():
                pltpu.make_async_copy(
                    stored.at[pl.ds(NB, 3 * NB), pl.ds(0, NB)], buf.at[k, pl.ds(2 * NB, 3 * NB), :], lsem.at[3]).wait()

    def x_rows(d, i):
        return (2 * (i % 8) + d) * CH

    def x_view(d, i):
        second = i // 8
        start = pl.multiple_of(NB + NB * second + x_rows(d, i), CH)
        return buf.at[slab + second * (2 - slab), pl.ds(start, CH), :]

    def x_copy(d, i):
        view = x_view(d, i)
        return remote(view, view, x_send.at[d], x_recv.at[d, i], (x_next, x_prev)[d])

    def xp_copy(d, i):
        target = other.at[i // 8, pl.ds(pl.multiple_of(x_rows(d, i), CH), CH), :]
        return remote(x_view(d, i), target, xp_send.at[d], xp_recv.at[d, i], partner)

    def p_copy(k, t, q, way):
        view = buf.at[k, pl.ds(pl.multiple_of((4 * q + t) * CH, CH), CH), :]
        return remote(view, view, p_send.at[k, t, way], p_recv.at[k, t, q], plane[way])

    def d_copy(k, t, q):
        view = buf.at[k, pl.ds(pl.multiple_of((4 * q + t) * CH, CH), CH), :]
        target = dx.at[k * (1 - core), pl.ds(pl.multiple_of((4 * (q - D0) + t) * CH, CH), CH), :]
        return remote(view, target, d_send.at[k, t], d_recv.at[k, t, q - D0], partner)

    depths, children = [], []
    for k in range(2):
        position = z * 4 + (y + 4 - k) % 4
        codes = [lookup(TREES[t], position) for t in range(4)]
        depths.append([code // 16 for code in codes])
        children.append([[(code // (1 << way)) % 2 == 1 for way in range(4)] for code in codes])
    has_diag = [core == 0, core >= 0]

    def step(s, _):
        for d in range(2):
            distance = x if d == 0 else (4 - x) % 4
            v = s - SKEW * distance - XDELAY * core
            w = s - SLOW * distance - XDELAY * core
            i = jnp.where(v < 8, v, 8 + (w - LATE) // EARLY)
            on_time = (v < 8) | ((w >= LATE) & (w % EARLY == 0))

            @pl.when((v >= 0) & (i < NX) & on_time)
            def _():
                @pl.when(distance > 0)
                def _():
                    x_copy(d, i).wait_recv()

                @pl.when(i > 0)
                def _():
                    xp_copy(d, i - 1).wait_send()

                xp_copy(d, i).start()

                @pl.when(distance < 3)
                def _():
                    @pl.when(i > 0)
                    def _():
                        x_copy(d, i - 1).wait_send()

                    x_copy(d, i).start()

        for k in range(2):
            for t in range(4):
                v = s - SKEW * depths[k][t]
                late = s - SLOW * depths[k][t]
                w = (late - LATE) // EARLY
                q_late = 8 + w
                if k == 1:
                    q_late = q_late - core * jnp.where(w < 3, 0, jnp.where(w < 7, 7, 4))
                q = jnp.where(v < DSTEP, v // EARLY, jnp.where(v < LATE, D0 + (v - DSTEP) // 2, q_late))
                early = (v >= 0) & (v < EARLY * D0) & (v % EARLY == 0)
                diag = (v >= DSTEP) & (v < LATE) & ((v - DSTEP) % 2 == 0) & (core == 0)
                active = early | diag | ((late >= LATE) & (late % EARLY == 0) & (q < NQ))
                in_diag = (q >= D0) & (q < D1)

                @pl.when(active)
                def _():
                    @pl.when(depths[k][t] > 0)
                    def _():
                        p_copy(k, t, q, 0).wait_recv()

                    for way in range(4):
                        @pl.when(children[k][t][way])
                        def _():
                            @pl.when(q > 0)
                            def _():
                                p_copy(k, t, q - 1, way).wait_send()

                            p_copy(k, t, q, way).start()

                    @pl.when(in_diag)
                    def _():
                        @pl.when(q > D0)
                        def _():
                            d_copy(k, t, q - 1).wait_send()

                        d_copy(k, t, q).start()
        return 0

    def take(k):
        for t in range(4):
            for j in range(D1 - D0):
                d_copy(k, t, D0 + j).wait_recv()

    lax.fori_loop(0, 12, step, 0)
    loaded()
    lax.fori_loop(12, FIRST, step, 0)

    ri = lax.broadcasted_iota(jnp.int32, (TB, TB), 0)
    ci = lax.broadcasted_iota(jnp.int32, (TB, TB), 1)
    n = NB // TB
    ld[...] = jnp.zeros_like(ld)

    @pl.when(core == 0)
    def _():
        b[0] = buf[0, pl.ds(NB, NB), :]

    @pl.when(core == 1)
    def _():
        take(0)
        b[0] = dx[0]

    def tile(g, _):
        half, blk = g // n, g % n

        @pl.when(g == n)
        def _():
            v0 = lower_tiles(b[0])

            @pl.when(core == 0)
            def _():
                take(1)
                u01[...] = jnp.dot(v0, buf[1, pl.ds(NB, NB), :], precision=HI, preferred_element_type=F32)
                b[1] = dx[0]

            @pl.when(core == 1)
            def _():
                take(1)
                u01[...] = jnp.dot(v0, dx[1], precision=HI, preferred_element_type=F32)
                b[1] = buf[1, pl.ds(NB, NB), :]

            s11[...] = u01[...].T
            b[1] -= jnp.dot(s11[...], u01[...], precision=HI, preferred_element_type=F32)

        base = pl.multiple_of(blk * TB, TB)
        rows = pl.ds(base, TB)
        t[:, :TB] = b[half, rows, rows]
        t[:, TB:] = jnp.where(ri == ci, 1.0, 0.0)
        begin = jnp.where(g < n, 3 * g, n + 2 * g)
        finish = begin + jnp.where((g < n) | (g == 2 * n - 1), 3, 2)

        def late_step(u, _):
            return step(FIRST + EARLY * u, 0)

        factor_tile(t, ld, lambda: late_step(begin, 0))
        w = jnp.where(ri >= ci, t[:, TB:], 0.0)
        ud[g] = jnp.where(ri <= ci, t[:, :TB], 0.0)
        b[half, rows, :] = mul6(split3(w), split3(b[half, rows, :]))
        b[half, rows, rows] = w
        done = b[half, rows, :]
        change = mul6(split3(done.T), split3(done))
        for i in range(1, n):
            @pl.when(blk < i)
            def _():
                b[half, TB * i : TB * i + TB, rows] = jnp.zeros((TB, TB), F32)
                b[half, TB * i : TB * i + TB, :] -= change[TB * i : TB * i + TB, :]

        lax.fori_loop(begin + 1, finish, late_step, 0)
        return 0

    lax.fori_loop(0, 2 * n, tile, 0)

    for d in range(2):
        distance = x if d == 0 else (4 - x) % 4
        xp_copy(d, NX - 1).wait_send()
        for i in range(NX):
            xp_copy(d, i).wait_recv()

        @pl.when(distance < 3)
        def _():
            x_copy(d, NX - 1).wait_send()
    for k in range(2):
        for t in range(4):
            for way in range(4):
                @pl.when(children[k][t][way])
                def _():
                    p_copy(k, t, NQ - 1, way).wait_send()

            @pl.when(has_diag[k])
            def _():
                d_copy(k, t, D1 - 1).wait_send()

    first, second = pl.ds(0, NB), pl.ds(NB, NB)
    outs = [
        (buf.at[pl.ds(0, 2), first, :], arow_out.at[:, first, :]),
        (buf.at[pl.ds(0, 2), pl.ds(2 * NB, 3 * NB), :], arow_out.at[:, pl.ds(NB, 3 * NB), :]),
        (buf.at[slab, second, :], acol_out.at[core, :, first]),
        (buf.at[2, pl.ds(2 * NB, NB), :], acol_out.at[core, :, second]),
        (other.at[0], acol_out.at[1 - core, :, first]),
        (other.at[1], acol_out.at[1 - core, :, second]),
        (u01, u01_out),
        (ud, ud_out),
        (b, b_out),
        (ld, ld_out),
    ]
    copies = [pltpu.make_async_copy(src, dst, lsem.at[index]) for index, (src, dst) in enumerate(outs)]
    for copy in copies:
        copy.start()
    for copy in copies:
        copy.wait()


def panels(stored):
    rows, cols = stored.shape
    n = NB // TB
    outs = ((2, rows, NB), (2, NB, cols), (2, NB, NB), (NB, NB), (2 * n, TB, TB), (8, 128))
    scratch = ((3, rows + NB, NB), (2, NB, NB), (2, NB, NB), (2, NB, NB), (NB, NB), (2 * n, TB, TB), (8, 128),
               (TB, 2 * TB), (NB, NB))
    dma = pltpu.SemaphoreType.DMA
    return pl.pallas_call(
        panel_kernel,
        name="gather_and_factor",
        out_shape=tuple(jax.ShapeDtypeStruct(s, F32) for s in outs),
        in_specs=[pl.BlockSpec(memory_space=pl.ANY)],
        out_specs=(pl.BlockSpec(memory_space=pl.ANY),) * len(outs),
        scratch_shapes=[pltpu.VMEM(s, F32) for s in scratch]
        + [
            dma((10,)),
            dma((2, NX)),
            dma((2, NX)),
            dma((2,)),
            dma((2,)),
            dma((2, 4, NQ)),
            dma((2, 4, 4)),
            dma((2, 4, D1 - D0)),
            dma((2, 4)),
        ],
        compiler_params=pltpu.CompilerParams(
            collective_id=0, has_side_effects=True, vmem_limit_bytes=60 << 20),
    )(stored)


def spread(value, k):
    return jnp.broadcast_to(value[k : k + 1, :], (8, 128))


def split3(value):
    high = value.astype(BF)
    rest = value - high.astype(F32)
    middle = rest.astype(BF)
    low = (rest - middle.astype(F32)).astype(BF)
    return high, middle, low


def split2(value):
    high = value.astype(BF)
    return high, (value - high.astype(F32)).astype(BF)


def mul6(a, b):
    lhs = jnp.concatenate([a[0], a[0], a[1], a[0], a[2], a[1]], 1)
    rhs = jnp.concatenate([b[0], b[1], b[0], b[2], b[0], b[1]], 0)
    return jnp.dot(lhs, rhs, preferred_element_type=F32)


def factor_tile(t, ld, between):
    sub = lax.broadcasted_iota(jnp.int32, (8, 128), 0)
    for p in range(8):
        r0 = 16 * p
        r = [[t[r0 + 8 * g : r0 + 8 * g + 8, 128 * h : 128 * h + 128] for h in range(2)] for g in range(2)]
        top = [jnp.broadcast_to(r[0][0][:, r0 + j : r0 + j + 1], (8, 128)) for j in range(8)]
        bot = [jnp.broadcast_to(r[1][0][:, r0 + j : r0 + j + 1], (8, 128)) for j in range(16)]
        piv = [jnp.ones((8, 128), F32), jnp.ones((8, 128), F32)]
        for k in range(16):
            g, kk = divmod(k, 8)
            pv = spread(top[k] if g == 0 else bot[k], kk)
            inv = 1.0 / pv
            piv[g] = jnp.where(sub == kk, pv, piv[g])
            mb = bot[k] * inv
            mt = top[k] * inv if g == 0 else None
            for j in range(k + 1, 16):
                s = spread(top[k], j) if j < 8 else spread(bot[k], j - 8)
                bot[j] = bot[j] - mb * s
                if j < 8:
                    top[j] = top[j] - mt * s
            for h in range(2):
                u = spread(r[g][h], kk)
                if g == 0:
                    r[0][h] = r[0][h] - jnp.where(sub > kk, mt, 0.0) * u
                    r[1][h] = r[1][h] - mb * u
                else:
                    r[1][h] = r[1][h] - jnp.where(sub > kk, mb, 0.0) * u
        ld[...] += jnp.log(piv[0]) + jnp.log(piv[1])
        rows = []
        for g in range(2):
            rs = lax.rsqrt(piv[g])
            rows.append([r[g][h] * rs for h in range(2)])
            for h in range(2):
                t[r0 + 8 * g : r0 + 8 * g + 8, 128 * h : 128 * h + 128] = rows[g][h]
        if p < 7:
            uh, um, ul = split3(jnp.concatenate([rows[0][0], rows[1][0]], 0))
            wh, wm, wl = split3(jnp.concatenate([rows[0][1], rows[1][1]], 0))
            lhs = jnp.concatenate([uh, uh, um, uh, ul, um], 0)
            rhs = jnp.concatenate(
                [jnp.concatenate([uh, um, uh, ul, uh, um], 0), jnp.concatenate([wh, wm, wh, wl, wh, wm], 0)], 1)
            upd = lax.dot_general(lhs, rhs, (((0,), (0,)), ((), ())), preferred_element_type=F32)
            t[r0 + 16 :, :] -= upd[r0 + 16 :, :]
        if p == 3:
            between()


def lower_tiles(b):
    ri = lax.broadcasted_iota(jnp.int32, (NB, NB), 0) // TB
    ci = lax.broadcasted_iota(jnp.int32, (NB, NB), 1) // TB
    return jnp.where(ri >= ci, b, 0.0)


def mul3(a, b, contract=((1,), (0,))):
    dims = (contract, ((), ()))
    dot = lambda p, q: lax.dot_general(p, q, dims, preferred_element_type=F32)
    return dot(a[0], b[0]) + (dot(a[0], b[1]) + dot(a[1], b[0]))


BT = ((1,), (1,))


def lower_factor(k, b, ud, out):
    n = NB // TB
    for i in range(n):
        for j in range(n):
            if i > j:
                tile = b[k, TB * j : TB * j + TB, TB * i : TB * i + TB].T
            elif i == j:
                tile = ud[k * n + i].T
            else:
                tile = jnp.zeros((TB, TB), F32)
            out[TB * i : TB * i + TB, TB * j : TB * j + TB] = tile


def update_kernel(m, arow, acol, b, u01, ud, ld, out, log_det, yh, yl, vh, vl, p):
    step = pl.program_id(0)
    row = lax.axis_index("row")
    col = lax.axis_index("col")

    half = NB // 2

    def times_lower(slot, a):
        short = [part[:, :half] for part in a]
        return jnp.concatenate([
            mul3(short, (vh[slot, :half, :half], vl[slot, :half, :half]), BT),
            mul3(a, (vh[slot, half:, :], vl[slot, half:, :]), BT)], 1)

    def lower_times(slot, a):
        short = [part[:half] for part in a]
        return jnp.concatenate([
            mul3((vh[slot, :half, :half], vl[slot, :half, :half]), short),
            mul3((vh[slot, half:, :], vl[slot, half:, :]), a)], 0)

    @pl.when(step == 0)
    def _():
        log_det[0, 0] = jnp.sum(ld[:, 0:1])
        for slot in range(2):
            vh[slot], vl[slot] = split2(lower_tiles(b[slot]))
        vh[2], vl[2] = split2(u01[...])
        for c in range(2):
            cols = pl.ds(c * NB, NB)
            y0 = lower_times(0, split2(acol[0, :, cols]))
            y0s = split2(y0)
            yh[:NB, cols], yl[:NB, cols] = y0s
            rest = acol[1, :, cols] - mul3((vh[2], vl[2]), y0s, ((0,), (0,)))
            yh[NB:, cols], yl[NB:, cols] = split2(lower_times(1, split2(rest)))

    p0 = times_lower(0, split2(arow[0]))
    p0s = split2(p0)
    rest = arow[1] - mul3(p0s, (vh[2], vl[2]))
    p1 = times_lower(1, split2(rest))
    p1s = split2(p1)
    p[0], p[1] = p0, p1
    for c in range(2):
        cols = pl.ds(c * NB, NB)
        out[:, cols] = m[:, cols] - (
            mul3(p0s, (yh[:NB, cols], yl[:NB, cols])) + mul3(p1s, (yh[NB:, cols], yl[NB:, cols])))

    first = step == 0

    @pl.when(first & (row < 2))
    def _():
        out[...] = jnp.zeros_like(out)

    @pl.when((col == 0) & ~(first & (row == 0)))
    def _():
        out[:, pl.ds(0, NB)] = p[0]

    @pl.when((col == 1) & ~(first & (row < 2)))
    def _():
        out[:, pl.ds(0, NB)] = p[1]

    @pl.when((col == 0) & first & (row == 0))
    def _():
        lower_factor(0, b, ud, out)

    @pl.when((col == 1) & first & (row == 1))
    def _():
        lower_factor(1, b, ud, out)


def update(stored, arow, acol, b, u01, ud, ld):
    rows, cols = stored.shape
    whole = lambda a: pl.BlockSpec(a.shape, lambda i: (0,) * a.ndim, pipeline_mode=pl.Buffered(1))
    return pl.pallas_call(
        update_kernel,
        name="update_remaining",
        grid=(rows // NB,),
        out_shape=(jax.ShapeDtypeStruct(stored.shape, F32), jax.ShapeDtypeStruct((1, 1), F32)),
        in_specs=[
            pl.BlockSpec((NB, cols), lambda i: (i, 0)),
            pl.BlockSpec((2, NB, NB), lambda i: (0, i, 0)),
        ]
        + [whole(a) for a in (acol, b, u01, ud, ld)],
        out_specs=(pl.BlockSpec((NB, cols), lambda i: (i, 0)), pl.BlockSpec(memory_space=pltpu.SMEM)),
        scratch_shapes=[
            pltpu.VMEM((2 * NB, cols), BF),
            pltpu.VMEM((2 * NB, cols), BF),
            pltpu.VMEM((3, NB, NB), BF),
            pltpu.VMEM((3, NB, NB), BF),
            pltpu.VMEM((2, NB, NB), F32),
        ],
        compiler_params=pltpu.CompilerParams(vmem_limit_bytes=60 << 20),
    )(stored, arow, acol, b, u01, ud, ld)


def per_device(stored):
    updated, log_det = update(stored, *panels(stored))
    return updated, log_det.reshape(())


def solution(mesh):
    placed = (P("row", "col"),)
    return jax.shard_map(
        per_device, mesh=mesh, in_specs=placed, out_specs=(P("row", "col"), P()), check_vma=False
    )
```
